128 devices in a mesh: groups: 4 (over y, x), seq: 16 (over z), head: 2 (over core).
Axes of the slice: x: 2, y: 2, z: 16, core: 2. Of those that a mesh axis runs over, the one named last changes fastest.
The devices are a block of a 8x8x16 slice.
Arguments:
- queries: bfloat16 [16384, 3584], P(('groups', 'seq'), 'head'), parts along dimension 0, may hold values from -30 to 30
- current_keys: bfloat16 [16384, 512], P(('groups', 'seq'), 'head'), parts along dimension 0, may hold values from -6 to 6
- current_values: bfloat16 [16384, 512], P(('groups', 'seq'), 'head'), parts along dimension 0, may hold values from -6 to 6
- stored_keys: bfloat16 [16384, 2, 512], P(('groups', 'seq'), None, 'head'), parts along dimension 0, may hold values from -22 to 22
- stored_values: bfloat16 [16384, 2, 512], P(('groups', 'seq'), None, 'head'), parts along dimension 0, may hold values from -6 to 6
- remap_table: int32 [3, 256], P(None, ('groups', 'seq')), parts along dimension 1, may hold values from 0 to 4095
- block_table: int32 [1024], P('groups'), parts along dimension 0, may hold values from 0 to 15, as said below
Outputs:
- attended: bfloat16 [16384, 3584], P(('groups', 'seq'), 'head'), parts along dimension 0
- paged_keys: bfloat16 [4, 1024, 2048], P('head', ('groups', 'seq')), parts along dimension 1
- paged_values: bfloat16 [4, 1024, 2048], P('head', ('groups', 'seq')), parts along dimension 1
The draws below stay inside these ranges and needn't reach their ends.
There are 4 independent parts, one for each index of `groups`. The reference program is written for one: setup_inputs(seed, part) draws one part's arguments, and reference() takes and returns one part's arrays. A program takes and returns all parts, laid end to end along the dimension named above; each array names one. Nothing has to cross between parts.
Inputs may be any that keep to these rules, and one draw needn't show every extreme that they name: `block_table`: the entries of the blocks b that share b modulo 16 are a permutation of 0 to 15.
All inputs are finite; a program needn't handle non-finite values.
Results may differ from the reference program's by a relative error of at most 0.012.
The reference program's roundings to bfloat16 on the way count: a program that leaves them out, or rounds other values in their place, can miss the bound.
Values may be sent and summed in bfloat16 or wider, within the bound.
A program may use at most 128 MiB of HBM per device.

```python
import jax
import jax.numpy as jnp
from jax import lax

HQ = 28
KEY_VALUE_HEADS = 4
HEAD_SIZE = 128
PRIOR_SEGMENTS = 2
PAGE_TOKENS = 16
QBLK = 64
QUERY_PER_KEY = 7
SEGMENT_TOKENS = 4096
NQB = 64
SEGMENT_PAGES = 256
OWNERS = 16
PAGES_DEV = 16


def draw_queries(key, part):
    rotary_base = jnp.clip(jax.random.normal(jax.random.fold_in(key, 1), (SEGMENT_TOKENS, HQ * HEAD_SIZE), jnp.float32), -6.0, 6.0) * 2.2
    return rotary_base.astype(jnp.bfloat16)


def draw_stored_keys(key, part):
    rotary_base = jnp.clip(jax.random.normal(jax.random.fold_in(key, 2), (SEGMENT_TOKENS, PRIOR_SEGMENTS, KEY_VALUE_HEADS * HEAD_SIZE), jnp.float32), -6.0, 6.0)
    return rotary_base.astype(jnp.bfloat16)


def draw_block_table(key, part):
    holder_keys = jax.random.split(jax.random.fold_in(key, 5), OWNERS)
    orders = jax.vmap(lambda single: jax.random.permutation(single, PAGES_DEV))(holder_keys)
    return orders.T.reshape(-1).astype(jnp.int32)


def touch_ends(entries, own_key, smallest, top_value):
    spot = [jax.random.randint(jax.random.fold_in(own_key, axis), (), 0, length) for axis, length in enumerate(entries.shape)]
    main_axis = entries.shape.index(max(entries.shape))
    beside = spot[:main_axis] + [(spot[main_axis] + 1) % entries.shape[main_axis]] + spot[main_axis + 1:]
    return entries.at[tuple(spot)].set(smallest).at[tuple(beside)].set(top_value)


def block_levels(own_key, dims, cuts, least, top_value):
    def one(dim, shards_of):
        steps = jax.random.uniform(jax.random.fold_in(jax.random.fold_in(own_key, 6), dim), (shards_of,), jnp.float32, least / len(cuts), top_value / len(cuts))
        return jnp.repeat(jnp.exp(steps), dims[dim] // shards_of).reshape((-1,) + (1,) * (len(dims) - dim - 1))

    gain = one(*cuts[0])
    for cut in cuts[1:]:
        gain = gain * one(*cut)
    return gain


def scatter_about(stream_key, extent, spread, most, cuts=(), kind=jnp.bfloat16):
    loudness = block_levels(stream_key, extent, cuts, -0.22, 0.18) if cuts else 1.0
    values = jax.random.normal(stream_key, extent, jnp.float32) * spread * loudness
    return jnp.minimum(jnp.maximum(values, -most), most).astype(kind)


def setup_inputs(seed: int = 0, part: int = 0) -> dict:
    key_list = jax.random.split(jax.random.key(seed), 8)
    part_splits = jax.random.split(jax.random.fold_in(key_list[7], part), 8)
    queries = draw_queries(jax.random.fold_in(jax.random.fold_in(key_list[7], part), 71), part)
    current_keys = scatter_about(part_splits[1], (SEGMENT_TOKENS, KEY_VALUE_HEADS * HEAD_SIZE), 1.0, 6.0, ((0, 16), (1, 2)))
    current_values = scatter_about(part_splits[2], (SEGMENT_TOKENS, KEY_VALUE_HEADS * HEAD_SIZE), 1.0, 6.0, ((0, 16), (1, 2)))
    stored_keys = draw_stored_keys(jax.random.fold_in(jax.random.fold_in(key_list[7], part), 71), part)
    stored_values = scatter_about(part_splits[4], (SEGMENT_TOKENS, PRIOR_SEGMENTS, KEY_VALUE_HEADS * HEAD_SIZE), 1.0, 6.0, ((0, 16), (2, 2)))
    remap_table = touch_ends(jax.random.randint(part_splits[5], (3, NQB), 0, SEGMENT_TOKENS), jax.random.fold_in(part_splits[5], 1), 0, SEGMENT_TOKENS - 1).astype(jnp.int32)
    block_table = draw_block_table(jax.random.fold_in(jax.random.fold_in(key_list[7], part), 71), part)
    return dict(queries=queries, current_keys=current_keys, current_values=current_values, stored_keys=stored_keys, stored_values=stored_values, remap_table=remap_table, block_table=block_table)


rope_base = 1000000.0
masked_value = -1e30


def apply_rotary(values, token_positions):
    half_dim = values.shape[-1] // 2
    frequency = rope_base ** (-2.0 * jnp.arange(half_dim, dtype=jnp.float32) / values.shape[-1])
    angles = token_positions.astype(jnp.float32)[:, None] * frequency[None, :]
    cos_table = jnp.cos(angles)[:, None, :]
    sin_table = jnp.sin(angles)[:, None, :]
    first_half = values[..., :half_dim]
    second_half = values[..., half_dim:]
    return jnp.concatenate([first_half * cos_table - second_half * sin_table, second_half * cos_table + first_half * sin_table], -1)


def paged_layout(cache_portion, block_table):
    page_blocks = cache_portion.reshape(SEGMENT_PAGES, PAGE_TOKENS, KEY_VALUE_HEADS, HEAD_SIZE).transpose(2, 0, 1, 3).reshape(KEY_VALUE_HEADS, SEGMENT_PAGES, PAGE_TOKENS * HEAD_SIZE)
    block_index = jnp.arange(SEGMENT_PAGES, dtype=jnp.int32)
    target = (block_index % OWNERS) * PAGES_DEV + block_table
    return jnp.zeros_like(page_blocks).at[:, target].set(page_blocks)


def reference(queries, current_keys, current_values, stored_keys, stored_values, remap_table, block_table):
    token_index = jnp.arange(SEGMENT_TOKENS, dtype=jnp.int32)
    token_positions = jnp.repeat(remap_table, QBLK, axis=1) + (token_index % QBLK)[None, :]
    query_single_float = queries.astype(jnp.float32).reshape(SEGMENT_TOKENS, HQ, HEAD_SIZE)
    rotary_output = [apply_rotary(query_single_float, token_positions[segment_kind_index]).astype(jnp.bfloat16).reshape(SEGMENT_TOKENS, KEY_VALUE_HEADS, QUERY_PER_KEY, HEAD_SIZE) for segment_kind_index in range(3)]
    score_scale = HEAD_SIZE ** -0.5
    value_portions = [stored_values[:, segment_number, :] for segment_number in range(PRIOR_SEGMENTS)] + [current_values]
    joined_values = jnp.concatenate(value_portions, 0).reshape((PRIOR_SEGMENTS + 1) * SEGMENT_TOKENS, KEY_VALUE_HEADS, HEAD_SIZE).astype(jnp.float32)
    query_block = min(256, SEGMENT_TOKENS)

    def one_block(block_number):
        first_row = block_number * query_block
        score_parts = []
        for segment_number in range(PRIOR_SEGMENTS):
            chosen = rotary_output[2] if segment_number < PRIOR_SEGMENTS - 1 else rotary_output[1]
            query_rows = lax.dynamic_slice_in_dim(chosen, first_row, query_block, 0).astype(jnp.float32)
            key_row_list = stored_keys[:, segment_number, :].reshape(SEGMENT_TOKENS, KEY_VALUE_HEADS, HEAD_SIZE).astype(jnp.float32)
            score_parts.append(jnp.einsum("qgrd,kgd->grqk", query_rows, key_row_list) * score_scale)
        query_rows = lax.dynamic_slice_in_dim(rotary_output[0], first_row, query_block, 0).astype(jnp.float32)
        key_row_list = current_keys.reshape(SEGMENT_TOKENS, KEY_VALUE_HEADS, HEAD_SIZE).astype(jnp.float32)
        intra = jnp.einsum("qgrd,kgd->grqk", query_rows, key_row_list) * score_scale
        allowed = token_index[None, :] <= (first_row + jnp.arange(query_block, dtype=jnp.int32))[:, None]
        score_parts.append(jnp.where(allowed[None, None], intra, masked_value))
        scores = jnp.concatenate(score_parts, -1)
        weights = jnp.exp(scores - jnp.max(scores, -1, keepdims=True))
        denom = jnp.sum(weights, -1)
        rounded = weights.astype(jnp.bfloat16).astype(jnp.float32)
        summed = jnp.einsum("grqk,kgd->qgrd", rounded, joined_values)
        result = summed / denom.transpose(2, 0, 1)[..., None]
        return result.astype(jnp.bfloat16).reshape(query_block, HQ * HEAD_SIZE)

    attended = lax.map(one_block, jnp.arange(SEGMENT_TOKENS // query_block, dtype=jnp.int32)).reshape(SEGMENT_TOKENS, HQ * HEAD_SIZE)
    paged_keys = paged_layout(stored_keys[:, PRIOR_SEGMENTS - 1, :], block_table)
    paged_values = paged_layout(stored_values[:, PRIOR_SEGMENTS - 1, :], block_table)
    return (attended, paged_keys, paged_values)
```

```python
import functools

import jax
import jax.numpy as jnp
import numpy as np
from jax import lax
from jax.experimental import pallas as pl
from jax.experimental.pallas import tpu as pltpu
from jax.sharding import PartitionSpec as P

HEAD = 128
PAGE = 16
QBLK = 64
ROPE_BASE = 1000000.0
MASKED = -1e30
MESH = pl.DeviceIdType.MESH
F32 = jnp.float32
BF16 = jnp.bfloat16
SCALE2 = float(HEAD**-0.5 * np.log2(np.e))


def kernel(
    n, groups, per,
    table_ref, remap_ref, freq_ref, q_ref, sk_ref, sv_ref, ck_ref, cv_ref,
    out_ref, pk_ref, pv_ref,
    kv, qrot, acc, m_ref, l_ref,
    local_sem, send_sem, recv_sem,
):
    me = lax.axis_index("seq")
    half = n // 2
    rows = q_ref.shape[0]
    width = groups * HEAD
    right, left = lax.rem(me + 1, n), lax.rem(me + n - 1, n)

    barrier = pltpu.get_barrier_semaphore()
    for neighbour in (left, right):
        pl.semaphore_signal(barrier, inc=1, device_id={"seq": neighbour}, device_id_type=MESH)

    def own(seg, side, g):
        stored, current = ((sk_ref, ck_ref), (sv_ref, cv_ref))[side]
        src = stored if seg < 2 else current
        col = (seg * width if seg < 2 else 0) + g * HEAD
        return pltpu.make_async_copy(
            src.at[:, pl.ds(col, HEAD)], kv.at[me, seg, side, g], local_sem.at[seg, side, g]
        )

    for seg in range(3):
        for side in range(2):
            for g in range(groups):
                own(seg, side, g).start()
    pl.semaphore_wait(barrier, 2)

    def ring(way, slot, seg, side):
        unit = kv.at[slot, seg, side]
        return pltpu.make_async_remote_copy(
            src_ref=unit,
            dst_ref=unit,
            send_sem=send_sem.at[way, slot, seg, side],
            recv_sem=recv_sem.at[slot, seg, side],
            device_id={"seq": (right, left)[way]},
            device_id_type=MESH,
        )

    for seg in range(3):
        for side in range(2):
            for g in range(groups):
                own(seg, side, g).wait()
            ring(0, me, seg, side).start()
            ring(1, me, seg, side).start()

    lanes = lax.broadcasted_iota(jnp.int32, (QBLK, HEAD), 1)
    rising = lax.broadcasted_iota(jnp.int32, (QBLK, HEAD), 0)
    freq = freq_ref[...]

    def rotate(step, _):
        kind = step // (rows // QBLK)
        blk = lax.rem(step, rows // QBLK)
        angle = (rising + remap_ref[kind, blk]).astype(F32) * freq
        cos = jnp.cos(angle)
        sin = jnp.sin(angle)
        sin = jnp.where(lanes < HEAD // 2, -sin, sin)
        at = pl.ds(pl.multiple_of(blk * QBLK, QBLK), QBLK)
        for h in range(groups * per):
            x = q_ref[at, h * HEAD : (h + 1) * HEAD].astype(F32)
            turned = x * cos + pltpu.roll(x, HEAD // 2, 1) * sin
            qrot[2 - kind, h, at, :] = turned.astype(BF16)
        return 0

    lax.fori_loop(0, 3 * (rows // QBLK), rotate, 0)

    m_ref[...] = jnp.full_like(m_ref, MASKED)
    l_ref[...] = jnp.zeros_like(l_ref)
    acc[...] = jnp.zeros_like(acc)

    def attend(slots, seg, masked=False):
        keys = [[kv[slot, seg, 0, g] for slot in slots] for g in range(groups)]
        values = [[kv[slot, seg, 1, g].T for slot in slots] for g in range(groups)]
        if masked:
            key = lax.broadcasted_iota(jnp.int32, (rows, rows), 0)
            tok = lax.broadcasted_iota(jnp.int32, (rows, rows), 1)
            allowed = key <= tok

        def scores(h):
            q = qrot[seg, h]
            parts = [
                lax.dot_general(k, q, (((1,), (1,)), ((), ())), preferred_element_type=F32)
                for k in keys[h // per]
            ]
            return [jnp.where(allowed, s, MASKED) for s in parts] if masked else parts

        def gather(h, weights, alpha):
            parts = [
                jnp.dot(vt, p, preferred_element_type=F32)
                for vt, p in zip(values[h // per], weights)
            ]
            acc[h] = acc[h] * alpha + functools.reduce(jnp.add, parts)

        ahead, behind = scores(0), None
        for h in range(groups * per):
            now = ahead
            if h + 1 < groups * per:
                ahead = scores(h + 1)
            m_old = m_ref[h]
            m_new = jnp.maximum(
                m_old, jnp.max(functools.reduce(jnp.maximum, now), axis=0, keepdims=True)
            )
            alpha = jnp.exp2((m_old - m_new) * SCALE2)
            weights = [jnp.exp2((s - m_new) * SCALE2) for s in now]
            m_ref[h] = m_new
            l_ref[h] = l_ref[h] * alpha + jnp.sum(
                functools.reduce(jnp.add, weights), axis=0, keepdims=True
            )
            if behind is not None:
                gather(*behind)
            behind = (h, [p.astype(BF16) for p in weights], alpha)
        gather(*behind)

    def first(seg, _):
        attend((me,), seg)
        return 0

    lax.fori_loop(0, 2, first, 0)
    attend((me,), 2, True)

    def step(t, _):
        def of_seg(seg, _):
            for way in range(2):
                slot = lax.rem(me + (n - t if way == 0 else t), n)
                for side in range(2):
                    ring(way, slot, seg, side).wait_recv()
                    if side == way:
                        ring(way, slot, seg, side).start()
                    else:
                        @pl.when(t < half - 1)
                        def _():
                            ring(way, slot, seg, side).start()

            up, down = lax.rem(me + n - t, n), lax.rem(me + t, n)
            up_counts = (seg < 2) | (up < me)
            down_counts = (seg < 2) | (down < me)

            @pl.when(up_counts & down_counts)
            def _():
                attend((up, down), seg)

            @pl.when(up_counts != down_counts)
            def _():
                attend((jnp.where(up_counts, up, down),), seg)

            return 0

        lax.fori_loop(0, 3, of_seg, 0)
        return 0

    lax.fori_loop(1, half, step, 0)

    far = lax.rem(me + half, n)

    def last(seg, _):
        for side in range(2):
            ring(side, far, seg, side).wait_recv()

        @pl.when((seg < 2) | (far < me))
        def _():
            attend((far,), seg)

        return 0

    lax.fori_loop(0, 3, last, 0)

    at = pl.ds(pl.multiple_of(me * PAGE, PAGE), PAGE)

    def page(s, _):
        def find(j, found):
            return jnp.maximum(found, jnp.where(table_ref[j * n + me] == s, j, 0))

        source = lax.fori_loop(0, n, find, 0)
        for g in range(groups):
            pk_ref[g, s] = kv[source, 1, 0, g, at, :]
            pv_ref[g, s] = kv[source, 1, 1, g, at, :]
        return 0

    lax.fori_loop(0, n, page, 0)

    for h in range(groups * per):
        out_ref[:, h * HEAD : (h + 1) * HEAD] = (acc[h] / l_ref[h]).T.astype(BF16)

    def drain(t, _):
        for way in range(2):
            slot = lax.rem(me + (n - t if way == 0 else t), n)
            for seg in range(3):
                for side in range(2):
                    if side == way:
                        ring(way, slot, seg, side).wait_send()
                    else:
                        @pl.when(t < half - 1)
                        def _():
                            ring(way, slot, seg, side).wait_send()
        return 0

    lax.fori_loop(0, half, drain, 0)


def shards(queries, current_keys, current_values, stored_keys, stored_values, remap_table, block_table, *, n):
    rows = queries.shape[0]
    groups = current_keys.shape[1] // HEAD
    heads = queries.shape[1] // HEAD
    d = np.arange(HEAD // 2, dtype=np.float32)
    freq = (np.float32(ROPE_BASE) ** (np.float32(-2.0) * d / np.float32(HEAD))).astype(np.float32)
    freq = jnp.asarray(np.concatenate([freq, freq])[None, :])
    flat = lambda a: a.reshape(rows, -1)
    smem = pl.BlockSpec(memory_space=pltpu.SMEM)
    vmem = pl.BlockSpec(memory_space=pltpu.VMEM)
    hbm = pl.BlockSpec(memory_space=pl.ANY)
    attended, pk, pv = pl.pallas_call(
        functools.partial(kernel, n, groups, heads // groups),
        out_shape=(
            jax.ShapeDtypeStruct(queries.shape, BF16),
            jax.ShapeDtypeStruct((groups, n, PAGE, HEAD), BF16),
            jax.ShapeDtypeStruct((groups, n, PAGE, HEAD), BF16),
        ),
        in_specs=[smem, smem, vmem, vmem, hbm, hbm, hbm, hbm],
        out_specs=(vmem, vmem, vmem),
        scratch_shapes=[
            pltpu.VMEM((n, 3, 2, groups, rows, HEAD), BF16),
            pltpu.VMEM((3, heads, rows, HEAD), BF16),
            pltpu.VMEM((heads, HEAD, rows), F32),
            pltpu.VMEM((heads, 1, rows), F32),
            pltpu.VMEM((heads, 1, rows), F32),
            pltpu.SemaphoreType.DMA((3, 2, groups)),
            pltpu.SemaphoreType.DMA((2, n, 3, 2)),
            pltpu.SemaphoreType.DMA((n, 3, 2)),
        ],
        compiler_params=pltpu.CompilerParams(
            collective_id=0, has_side_effects=True, vmem_limit_bytes=60 * 1024 * 1024
        ),
    )(
        block_table, remap_table, freq, queries,
        flat(stored_keys), flat(stored_values), current_keys, current_values,
    )
    return attended, pk.reshape(groups, n, -1), pv.reshape(groups, n, -1)


def solution(mesh):
    both = ("groups", "seq")
    in_specs = (
        P(both, "head"), P(both, "head"), P(both, "head"),
        P(both, None, "head"), P(both, None, "head"),
        P(None, both), P("groups"),
    )
    out_specs = (P(both, "head"), P("head", both, None), P("head", both, None))
    return jax.shard_map(
        functools.partial(shards, n=mesh.shape["seq"]),
        mesh=mesh, in_specs=in_specs, out_specs=out_specs, check_vma=False,
    )
```

```python
import functools

import jax
import jax.numpy as jnp
import numpy as np
from jax import lax
from jax.experimental import pallas as pl
from jax.experimental.pallas import tpu as pltpu
from jax.sharding import PartitionSpec as P

HEAD = 128
PAGE = 16
QBLK = 64
ROPE_BASE = 1000000.0
MASKED = -1e30
MESH = pl.DeviceIdType.MESH
F32 = jnp.float32
BF16 = jnp.bfloat16
SCALE2 = float(HEAD**-0.5 * np.log2(np.e))


def kernel(
    n, groups, per,
    table_ref, remap_ref, freq_ref, q_hbm, sk_hbm, sv_hbm, ck_hbm, cv_hbm,
    out_ref, pk_ref, pv_ref,
    kv, q_ref, raw, qrot, acc, m_ref, l_ref, pages, turned_pages, source_ref,
    own_sem, raw_sem, q_sem, send_sem, recv_sem,
):
    me = lax.axis_index("seq")
    half = n // 2
    rows = q_ref.shape[0]
    heads = groups * per
    right, left = lax.rem(me + 1, n), lax.rem(me + n - 1, n)

    def current(side, g):
        return pltpu.make_async_copy(
            (ck_hbm, cv_hbm)[side].at[:, pl.ds(g * HEAD, HEAD)], kv.at[me, 2, side, g], own_sem.at[side, g]
        )

    def stored(side):
        return pltpu.make_async_copy((sk_hbm, sv_hbm)[side], raw.at[side], raw_sem.at[side])

    all_queries = pltpu.make_async_copy(q_hbm, q_ref, q_sem)

    barrier = pltpu.get_barrier_semaphore()
    for neighbour in (left, right):
        pl.semaphore_signal(barrier, inc=1, device_id={"seq": neighbour}, device_id_type=MESH)
    for side in range(2):
        for g in range(groups):
            current(side, g).start()
    for side in range(2):
        stored(side).start()
    all_queries.start()

    def ring(way, slot, seg, side):
        unit = kv.at[slot, seg, side]
        return pltpu.make_async_remote_copy(
            src_ref=unit,
            dst_ref=unit,
            send_sem=send_sem.at[way, slot, seg, side],
            recv_sem=recv_sem.at[slot, seg, side],
            device_id={"seq": (right, left)[way]},
            device_id_type=MESH,
        )

    def wanted(way, slot, seg, to):
        return (seg < 2) | ((slot < to) if way == 0 else (slot + 1 < half))

    def goes_on(way, t, slot, seg, side):
        if side == way:
            return True
        near = t < half - 1
        return near | ((seg == 2) & (slot == half - 1)) if way == 0 else near

    def send_own(seg):
        for side in range(2):
            for way in range(2):
                @pl.when(wanted(way, me, seg, right))
                def _():
                    ring(way, me, seg, side).start()

    for side in range(2):
        for g in range(groups):
            current(side, g).wait()
    pl.semaphore_wait(barrier, 2)
    send_own(2)

    for side in range(2):
        stored(side).wait()
        both = raw[side].astype(F32)
        for seg in range(2):
            for g in range(groups):
                kv[me, seg, side, g] = both[:, seg, g * HEAD : (g + 1) * HEAD].astype(BF16)

    def find(s, _):
        source_ref[s] = lax.fori_loop(
            0, n, lambda j, found: jnp.maximum(found, jnp.where(table_ref[j * n + me] == s, j, 0)), 0
        )
        return 0

    lax.fori_loop(0, n, find, 0)
    for seg in (1, 0):
        send_own(seg)

    lanes = lax.broadcasted_iota(jnp.int32, (QBLK, HEAD), 1)
    rising = lax.broadcasted_iota(jnp.int32, (QBLK, HEAD), 0)
    freq = freq_ref[...]
    all_queries.wait()

    def rotate(step, _):
        kind = step // (rows // QBLK)
        blk = lax.rem(step, rows // QBLK)
        angle = (rising + remap_ref[kind, blk]).astype(F32) * freq
        cos = jnp.cos(angle)
        sin = jnp.sin(angle)
        sin = jnp.where(lanes < HEAD // 2, -sin, sin)
        at = pl.ds(pl.multiple_of(blk * QBLK, QBLK), QBLK)
        for h in range(heads):
            x = q_ref[at, h * HEAD : (h + 1) * HEAD].astype(F32)
            turned = x * cos + pltpu.roll(x, HEAD // 2, 1) * sin
            qrot[2 - kind, h, at, :] = turned.astype(BF16)
        return 0

    lax.fori_loop(0, 3 * (rows // QBLK), rotate, 0)

    m_ref[...] = jnp.full_like(m_ref, MASKED)
    l_ref[...] = jnp.zeros_like(l_ref)
    acc[...] = jnp.zeros_like(acc)

    def attend(slots, seg, masked=False, finish=False):
        keys = [[kv[slot, seg, 0, g] for slot in slots] for g in range(groups)]
        values = [[kv[slot, seg, 1, g].T for slot in slots] for g in range(groups)]
        if masked:
            key = lax.broadcasted_iota(jnp.int32, (rows, rows), 0)
            tok = lax.broadcasted_iota(jnp.int32, (rows, rows), 1)
            allowed = key <= tok

        def scores(h):
            q = qrot[seg, h]
            parts = [
                lax.dot_general(k, q, (((1,), (1,)), ((), ())), preferred_element_type=F32)
                for k in keys[h // per]
            ]
            return [jnp.where(allowed, s, MASKED) for s in parts] if masked else parts

        def gather(h, weights, alpha):
            parts = [
                jnp.dot(vt, p, preferred_element_type=F32)
                for vt, p in zip(values[h // per], weights)
            ]
            total = acc[h] * alpha + functools.reduce(jnp.add, parts)
            if finish:
                out_ref[:, h * HEAD : (h + 1) * HEAD] = (total / l_ref[h]).T.astype(BF16)
            else:
                acc[h] = total

        ahead, behind = scores(0), None
        for h in range(heads):
            now = ahead
            if h + 1 < heads:
                ahead = scores(h + 1)
            m_old = m_ref[h]
            m_new = jnp.maximum(
                m_old, jnp.max(functools.reduce(jnp.maximum, now), axis=0, keepdims=True)
            )
            alpha = jnp.exp2((m_old - m_new) * SCALE2)
            weights = [jnp.exp2((s - m_new) * SCALE2) for s in now]
            m_ref[h] = m_new
            l_ref[h] = l_ref[h] * alpha + jnp.sum(
                functools.reduce(jnp.add, weights), axis=0, keepdims=True
            )
            if behind is not None:
                gather(*behind)
            behind = (h, [p.astype(BF16) for p in weights], alpha)
        gather(*behind)

    page_rows = pl.ds(pl.multiple_of(me * PAGE, PAGE), PAGE)

    def keep_page(slot):
        for side in range(2):
            for g in range(groups):
                pages[slot, side, g] = kv[slot, 1, side, g, page_rows, :]

    def first(seg, _):
        attend((me,), seg)
        return 0

    keep_page(me)
    lax.fori_loop(0, 2, first, 0)
    attend((me,), 2, True)

    def step(t, _):
        up, down = lax.rem(me + n - t, n), lax.rem(me + t, n)

        def of_seg(i, _):
            seg = 2 - i
            for side in range(2):
                for way in range(2):
                    slot = (up, down)[way]

                    @pl.when(wanted(way, slot, seg, me))
                    def _():
                        ring(way, slot, seg, side).wait_recv()

                    @pl.when(wanted(way, slot, seg, right) & goes_on(way, t, slot, seg, side))
                    def _():
                        ring(way, slot, seg, side).start()

            @pl.when(seg == 1)
            def _():
                keep_page(up)
                keep_page(down)

            up_counts = (seg < 2) | (up < me)
            down_counts = (seg < 2) | (down < me)

            @pl.when(up_counts & down_counts)
            def _():
                attend((up, down), seg)

            @pl.when(up_counts != down_counts)
            def _():
                attend((jnp.where(up_counts, up, down),), seg)

            return 0

        lax.fori_loop(0, 3, of_seg, 0)
        return 0

    lax.fori_loop(1, half, step, 0)

    far = lax.rem(me + half, n)

    def last(i, _):
        seg = 2 - i

        @pl.when((seg < 2) | (far < me))
        def _():
            for side in range(2):
                ring(side, far, seg, side).wait_recv()
            attend((far,), seg)

        return 0

    lax.fori_loop(0, 2, last, 0)
    keep_page(far)

    def place(s, _):
        source = source_ref[s]
        at = pl.ds(pl.multiple_of(s * PAGE, PAGE), PAGE)
        for side in range(2):
            for g in range(groups):
                turned_pages[side, g, at, :] = pages[source, side, g].astype(F32)
        return 0

    lax.fori_loop(0, n, place, 0)
    for side, ref in enumerate((pk_ref, pv_ref)):
        for g in range(groups):
            for t in range(PAGE):
                ref[g, :, t * HEAD : (t + 1) * HEAD] = turned_pages[
                    side, g, pl.ds(t, n, stride=PAGE), :
                ].astype(BF16)

    for side in range(2):
        ring(side, far, 0, side).wait_recv()
    attend((far,), 0, finish=True)

    def drain(t, _):
        def of_seg(seg, _):
            for way in range(2):
                slot = lax.rem(me + (n - t if way == 0 else t), n)
                for side in range(2):
                    @pl.when(wanted(way, slot, seg, right) & goes_on(way, t, slot, seg, side))
                    def _():
                        ring(way, slot, seg, side).wait_send()
            return 0

        lax.fori_loop(0, 3, of_seg, 0)
        return 0

    lax.fori_loop(0, half, drain, 0)


def shards(queries, current_keys, current_values, stored_keys, stored_values, remap_table, block_table, *, n):
    rows = queries.shape[0]
    groups = current_keys.shape[1] // HEAD
    heads = queries.shape[1] // HEAD
    d = np.arange(HEAD // 2, dtype=np.float32)
    freq = (np.float32(ROPE_BASE) ** (np.float32(-2.0) * d / np.float32(HEAD))).astype(np.float32)
    freq = jnp.asarray(np.concatenate([freq, freq])[None, :])
    smem = pl.BlockSpec(memory_space=pltpu.SMEM)
    vmem = pl.BlockSpec(memory_space=pltpu.VMEM)
    hbm = pl.BlockSpec(memory_space=pltpu.HBM)
    paged = pltpu.VMEM((groups, n, PAGE * HEAD), BF16)
    return pl.pallas_call(
        functools.partial(kernel, n, groups, heads // groups),
        out_shape=(pltpu.VMEM(queries.shape, BF16), paged, paged),
        in_specs=[smem, smem, vmem, hbm, hbm, hbm, hbm, hbm],
        out_specs=(vmem, vmem, vmem),
        scratch_shapes=[
            pltpu.VMEM((n, 3, 2, groups, rows, HEAD), BF16),
            pltpu.VMEM(queries.shape, BF16),
            pltpu.VMEM((2, *stored_keys.shape), BF16),
            pltpu.VMEM((3, heads, rows, HEAD), BF16),
            pltpu.VMEM((heads, HEAD, rows), F32),
            pltpu.VMEM((heads, 1, rows), F32),
            pltpu.VMEM((heads, 1, rows), F32),
            pltpu.VMEM((n, 2, groups, PAGE, HEAD), BF16),
            pltpu.VMEM((2, groups, n * PAGE, HEAD), F32),
            pltpu.SMEM((n,), jnp.int32),
            pltpu.SemaphoreType.DMA((2, groups)),
            pltpu.SemaphoreType.DMA((2,)),
            pltpu.SemaphoreType.DMA,
            pltpu.SemaphoreType.DMA((2, n, 3, 2)),
            pltpu.SemaphoreType.DMA((n, 3, 2)),
        ],
        compiler_params=pltpu.CompilerParams(
            collective_id=0, has_side_effects=True, vmem_limit_bytes=58 * 1024 * 1024
        ),
    )(
        block_table, remap_table, freq, queries,
        stored_keys, stored_values, current_keys, current_values,
    )


def solution(mesh):
    both = ("groups", "seq")
    in_specs = (
        P(both, "head"), P(both, "head"), P(both, "head"),
        P(both, None, "head"), P(both, None, "head"),
        P(None, both), P("groups"),
    )
    out_specs = (P(both, "head"), P("head", both, None), P("head", both, None))
    return jax.shard_map(
        functools.partial(shards, n=mesh.shape["seq"]),
        mesh=mesh, in_specs=in_specs, out_specs=out_specs, check_vma=False,
    )
```

```python
import functools

import jax
import jax.numpy as jnp
import numpy as np
from jax import lax
from jax.experimental import pallas as pl
from jax.experimental.pallas import tpu as pltpu
from jax.sharding import PartitionSpec as P

HEAD = 128
PAGE = 16
QBLK = 64
ROPE_BASE = 1000000.0
MASKED = -1e30
MESH = pl.DeviceIdType.MESH
F32 = jnp.float32
BF16 = jnp.bfloat16
SCALE2 = float(HEAD**-0.5 * np.log2(np.e))


def kernel(
    n, groups, per,
    table_hbm, remap_hbm, freq_hbm, q_hbm, sk_hbm, sv_hbm, ck_hbm, cv_hbm,
    out_ref, pk_ref, pv_ref,
    table_ref, remap_ref, freq_ref, kv, q_ref, raw, qrot, acc, m_ref, l_ref, pages, turned_pages, source_ref,
    small_sem, own_sem, raw_sem, q_sem, send_sem, recv_sem, far_send, far_recv,
):
    me = lax.axis_index("seq")
    half = n // 2
    rows = q_ref.shape[0]
    heads = groups * per
    right, left = lax.rem(me + 1, n), lax.rem(me + n - 1, n)

    def current(side, g):
        return pltpu.make_async_copy(
            (ck_hbm, cv_hbm)[side].at[:, pl.ds(g * HEAD, HEAD)], kv.at[me, 2, side, g], own_sem.at[side, g]
        )

    def stored(side):
        return pltpu.make_async_copy((sk_hbm, sv_hbm)[side], raw.at[side], raw_sem.at[side])

    all_queries = pltpu.make_async_copy(q_hbm, q_ref, q_sem)
    small = [
        pltpu.make_async_copy(src, dst, small_sem.at[i])
        for i, (src, dst) in enumerate(
            ((table_hbm, table_ref), (remap_hbm, remap_ref), (freq_hbm, freq_ref))
        )
    ]

    barrier = pltpu.get_barrier_semaphore()
    for neighbour in (left, right):
        pl.semaphore_signal(barrier, inc=1, device_id={"seq": neighbour}, device_id_type=MESH)
    for side in range(2):
        for g in range(groups):
            current(side, g).start()
    for side in range(2):
        stored(side).start()
    for copy in small:
        copy.start()
    all_queries.start()

    def ring(way, slot, seg, side):
        unit = kv.at[slot, seg, side]
        return pltpu.make_async_remote_copy(
            src_ref=unit,
            dst_ref=unit,
            send_sem=send_sem.at[way, slot, seg, side],
            recv_sem=recv_sem.at[slot, seg, side],
            device_id={"seq": (right, left)[way]},
            device_id_type=MESH,
        )

    def part(way, slot, side, g):
        unit = kv.at[slot, 0, side, g]
        return pltpu.make_async_remote_copy(
            src_ref=unit,
            dst_ref=unit,
            send_sem=far_send.at[way, side, g],
            recv_sem=far_recv.at[side, g],
            device_id={"seq": (right, left)[way]},
            device_id_type=MESH,
        )

    def wanted(way, slot, seg, to):
        return (seg < 2) | ((slot < to) if way == 0 else (slot + 1 < half))

    def from_left(to, seg, side):
        if side == 0:
            return (to < half) | (to >= n - 2)
        return (to < half - 2) | ((to == n - 1) & (seg == 2))

    def goes_on(way, t, seg, side):
        last = from_left(right, seg, side) if way == 0 else jnp.logical_not(from_left(left, seg, side))
        return (t < half - 1) | last

    def send_own(seg):
        for side in range(2):
            for way in range(2):
                @pl.when(wanted(way, me, seg, right))
                def _():
                    ring(way, me, seg, side).start()

    for side in range(2):
        for g in range(groups):
            current(side, g).wait()
    pl.semaphore_wait(barrier, 2)
    send_own(2)

    for side in range(2):
        stored(side).wait()
        both = raw[side].astype(F32)
        for seg in range(2):
            for g in range(groups):
                kv[me, seg, side, g] = both[:, seg, g * HEAD : (g + 1) * HEAD].astype(BF16)

    for copy in small:
        copy.wait()

    def find(s, _):
        source_ref[s] = lax.fori_loop(
            0, n, lambda j, found: jnp.maximum(found, jnp.where(table_ref[j * n + me] == s, j, 0)), 0
        )
        return 0

    lax.fori_loop(0, n, find, 0)
    for seg in (1, 0):
        send_own(seg)

    lanes = lax.broadcasted_iota(jnp.int32, (QBLK, HEAD), 1)
    rising = lax.broadcasted_iota(jnp.int32, (QBLK, HEAD), 0)
    freq = freq_ref[...]
    all_queries.wait()

    def rotate(step, _):
        kind = step // (rows // QBLK)
        blk = lax.rem(step, rows // QBLK)
        angle = (rising + remap_ref[kind, blk]).astype(F32) * freq
        cos = jnp.cos(angle)
        sin = jnp.sin(angle)
        sin = jnp.where(lanes < HEAD // 2, -sin, sin)
        at = pl.ds(pl.multiple_of(blk * QBLK, QBLK), QBLK)
        for h in range(heads):
            x = q_ref[at, h * HEAD : (h + 1) * HEAD].astype(F32)
            turned = x * cos + pltpu.roll(x, HEAD // 2, 1) * sin
            qrot[2 - kind, h, at, :] = turned.astype(BF16)
        return 0

    lax.fori_loop(0, 3 * (rows // QBLK), rotate, 0)

    m_ref[...] = jnp.full_like(m_ref, MASKED)
    l_ref[...] = jnp.zeros_like(l_ref)
    acc[...] = jnp.zeros_like(acc)

    def attend(slots, seg, masked=False, finish=False, only=None):
        chosen = range(groups) if only is None else (only,)
        hs = range(chosen[0] * per, (chosen[-1] + 1) * per)
        keys = {g: [kv[slot, seg, 0, g] for slot in slots] for g in chosen}
        values = {g: [kv[slot, seg, 1, g].T for slot in slots] for g in chosen}
        if masked:
            key = lax.broadcasted_iota(jnp.int32, (rows, rows), 0)
            tok = lax.broadcasted_iota(jnp.int32, (rows, rows), 1)
            allowed = key <= tok

        def scores(h):
            q = qrot[seg, h]
            parts = [
                lax.dot_general(k, q, (((1,), (1,)), ((), ())), preferred_element_type=F32)
                for k in keys[h // per]
            ]
            return [jnp.where(allowed, s, MASKED) for s in parts] if masked else parts

        def gather(h, weights, alpha):
            parts = [
                jnp.dot(vt, p, preferred_element_type=F32)
                for vt, p in zip(values[h // per], weights)
            ]
            total = acc[h] * alpha + functools.reduce(jnp.add, parts)
            if finish:
                out_ref[:, h * HEAD : (h + 1) * HEAD] = (total / l_ref[h]).T.astype(BF16)
            else:
                acc[h] = total

        ahead, behind = scores(hs[0]), None
        for h in hs:
            now = ahead
            if h + 1 in hs:
                ahead = scores(h + 1)
            m_old = m_ref[h]
            m_new = jnp.maximum(
                m_old, jnp.max(functools.reduce(jnp.maximum, now), axis=0, keepdims=True)
            )
            alpha = jnp.exp2((m_old - m_new) * SCALE2)
            weights = [jnp.exp2((s - m_new) * SCALE2) for s in now]
            m_ref[h] = m_new
            l_ref[h] = l_ref[h] * alpha + jnp.sum(
                functools.reduce(jnp.add, weights), axis=0, keepdims=True
            )
            if behind is not None:
                gather(*behind)
            behind = (h, [p.astype(BF16) for p in weights], alpha)
        gather(*behind)

    page_rows = pl.ds(pl.multiple_of(me * PAGE, PAGE), PAGE)

    def keep_page(slot):
        for side in range(2):
            for g in range(groups):
                pages[slot, side, g] = kv[slot, 1, side, g, page_rows, :]

    def first(seg, _):
        attend((me,), seg)
        return 0

    keep_page(me)
    lax.fori_loop(0, 2, first, 0)
    attend((me,), 2, True)

    def step(t, _):
        up, down = lax.rem(me + n - t, n), lax.rem(me + t, n)

        def of_seg(i, _):
            seg = 2 - i
            for side in range(2):
                for way in range(2):
                    slot = (up, down)[way]

                    @pl.when(wanted(way, slot, seg, me))
                    def _():
                        ring(way, slot, seg, side).wait_recv()

                    sends = wanted(way, slot, seg, right) & goes_on(way, t, seg, side)
                    split = (t == half - 1) & (seg == 0)

                    @pl.when(sends & jnp.logical_not(split))
                    def _():
                        ring(way, slot, seg, side).start()

                    @pl.when(sends & split)
                    def _():
                        for g in range(groups):
                            part(way, slot, side, g).start()

            @pl.when(seg == 1)
            def _():
                keep_page(up)
                keep_page(down)

            up_counts = (seg < 2) | (up < me)
            down_counts = (seg < 2) | (down < me)

            @pl.when(up_counts & down_counts)
            def _():
                attend((up, down), seg)

            @pl.when(up_counts != down_counts)
            def _():
                attend((jnp.where(up_counts, up, down),), seg)

            return 0

        lax.fori_loop(0, 3, of_seg, 0)
        return 0

    lax.fori_loop(1, half, step, 0)

    far = lax.rem(me + half, n)

    def last(i, _):
        seg = 2 - i

        @pl.when((seg < 2) | (far < me))
        def _():
            for side in range(2):
                ring(side, far, seg, side).wait_recv()
            attend((far,), seg)

        return 0

    lax.fori_loop(0, 2, last, 0)
    keep_page(far)

    def place(s, _):
        source = source_ref[s]
        at = pl.ds(pl.multiple_of(s * PAGE, PAGE), PAGE)
        for side in range(2):
            for g in range(groups):
                turned_pages[side, g, at, :] = pages[source, side, g].astype(F32)
        return 0

    lax.fori_loop(0, n, place, 0)
    for side, ref in enumerate((pk_ref, pv_ref)):
        for g in range(groups):
            for t in range(PAGE):
                ref[g, :, t * HEAD : (t + 1) * HEAD] = turned_pages[
                    side, g, pl.ds(t, n, stride=PAGE), :
                ].astype(BF16)

    for g in range(groups):
        for side in range(2):
            part(side, far, side, g).wait_recv()
        attend((far,), 0, finish=True, only=g)

    def drain(t, _):
        def of_seg(seg, _):
            for way in range(2):
                slot = lax.rem(me + (n - t if way == 0 else t), n)
                for side in range(2):
                    sends = wanted(way, slot, seg, right) & goes_on(way, t, seg, side)
                    split = (t == half - 1) & (seg == 0)

                    @pl.when(sends & jnp.logical_not(split))
                    def _():
                        ring(way, slot, seg, side).wait_send()

                    @pl.when(sends & split)
                    def _():
                        for g in range(groups):
                            part(way, slot, side, g).wait_send()
            return 0

        lax.fori_loop(0, 3, of_seg, 0)
        return 0

    lax.fori_loop(0, half, drain, 0)


def shards(queries, current_keys, current_values, stored_keys, stored_values, remap_table, block_table, *, n):
    rows = queries.shape[0]
    groups = current_keys.shape[1] // HEAD
    heads = queries.shape[1] // HEAD
    d = np.arange(HEAD // 2, dtype=np.float32)
    freq = (np.float32(ROPE_BASE) ** (np.float32(-2.0) * d / np.float32(HEAD))).astype(np.float32)
    freq = jnp.asarray(np.concatenate([freq, freq])[None, :])
    vmem = pl.BlockSpec(memory_space=pltpu.VMEM)
    hbm = pl.BlockSpec(memory_space=pltpu.HBM)
    paged = pltpu.VMEM((groups, n, PAGE * HEAD), BF16)
    return pl.pallas_call(
        functools.partial(kernel, n, groups, heads // groups),
        out_shape=(pltpu.VMEM(queries.shape, BF16), paged, paged),
        in_specs=[hbm] * 8,
        out_specs=(vmem, vmem, vmem),
        scratch_shapes=[
            pltpu.SMEM(block_table.shape, jnp.int32),
            pltpu.SMEM(remap_table.shape, jnp.int32),
            pltpu.VMEM(freq.shape, F32),
            pltpu.VMEM((n, 3, 2, groups, rows, HEAD), BF16),
            pltpu.VMEM(queries.shape, BF16),
            pltpu.VMEM((2, *stored_keys.shape), BF16),
            pltpu.VMEM((3, heads, rows, HEAD), BF16),
            pltpu.VMEM((heads, HEAD, rows), F32),
            pltpu.VMEM((heads, 1, rows), F32),
            pltpu.VMEM((heads, 1, rows), F32),
            pltpu.VMEM((n, 2, groups, PAGE, HEAD), BF16),
            pltpu.VMEM((2, groups, n * PAGE, HEAD), F32),
            pltpu.SMEM((n,), jnp.int32),
            pltpu.SemaphoreType.DMA((3,)),
            pltpu.SemaphoreType.DMA((2, groups)),
            pltpu.SemaphoreType.DMA((2,)),
            pltpu.SemaphoreType.DMA,
            pltpu.SemaphoreType.DMA((2, n, 3, 2)),
            pltpu.SemaphoreType.DMA((n, 3, 2)),
            pltpu.SemaphoreType.DMA((2, 2, groups)),
            pltpu.SemaphoreType.DMA((2, groups)),
        ],
        compiler_params=pltpu.CompilerParams(
            collective_id=0, has_side_effects=True, vmem_limit_bytes=58 * 1024 * 1024
        ),
    )(
        block_table, remap_table, freq, queries,
        stored_keys, stored_values, current_keys, current_values,
    )


def solution(mesh):
    both = ("groups", "seq")
    in_specs = (
        P(both, "head"), P(both, "head"), P(both, "head"),
        P(both, None, "head"), P(both, None, "head"),
        P(None, both), P("groups"),
    )
    out_specs = (P(both, "head"), P("head", both, None), P("head", both, None))
    return jax.shard_map(
        functools.partial(shards, n=mesh.shape["seq"]),
        mesh=mesh, in_specs=in_specs, out_specs=out_specs, check_vma=False,
    )
```

```python
import functools

import jax
import jax.numpy as jnp
import numpy as np
from jax import lax
from jax.experimental import pallas as pl
from jax.experimental.pallas import tpu as pltpu
from jax.sharding import PartitionSpec as P

HEAD = 128
PAGE = 16
QBLK = 64
ROPE_BASE = 1000000.0
MASKED = -1e30
MESH = pl.DeviceIdType.MESH
F32 = jnp.float32
BF16 = jnp.bfloat16
SCALE2 = float(HEAD**-0.5 * np.log2(np.e))


def kernel(
    n, groups, per,
    table_hbm, remap_hbm, freq_hbm, q_hbm, sk_hbm, sv_hbm, ck_hbm, cv_hbm,
    out_ref, pk_ref, pv_ref,
    table_ref, remap_ref, freq_ref, kv, q_ref, raw, qrot, acc, m_ref, l_ref, pages, turned_pages, source_ref,
    small_sem, own_sem, raw_sem, q_sem, send_sem, recv_sem, far_send, far_recv,
):
    me = lax.axis_index("seq")
    half = n // 2
    rows = q_ref.shape[0]
    heads = groups * per
    right, left = lax.rem(me + 1, n), lax.rem(me + n - 1, n)

    def current(side, g):
        return pltpu.make_async_copy(
            (ck_hbm, cv_hbm)[side].at[:, pl.ds(g * HEAD, HEAD)], kv.at[me, 2, side, g], own_sem.at[side, g]
        )

    def stored(side):
        return pltpu.make_async_copy((sk_hbm, sv_hbm)[side], raw.at[side], raw_sem.at[side])

    all_queries = pltpu.make_async_copy(q_hbm, q_ref, q_sem)
    small = [
        pltpu.make_async_copy(src, dst, small_sem.at[i])
        for i, (src, dst) in enumerate(
            ((table_hbm, table_ref), (remap_hbm, remap_ref), (freq_hbm, freq_ref))
        )
    ]

    barrier = pltpu.get_barrier_semaphore()
    for neighbour in (left, right):
        pl.semaphore_signal(barrier, inc=1, device_id={"seq": neighbour}, device_id_type=MESH)
    for side in range(2):
        for g in range(groups):
            current(side, g).start()
    for side in range(2):
        stored(side).start()
    for copy in small:
        copy.start()
    all_queries.start()

    def send(unit, way, send_sem, recv_sem):
        return pltpu.make_async_remote_copy(
            src_ref=unit,
            dst_ref=unit,
            send_sem=send_sem,
            recv_sem=recv_sem,
            device_id={"seq": (right, left)[way]},
            device_id_type=MESH,
        )

    def ring(way, slot, seg):
        return send(kv.at[slot, seg], way, send_sem.at[way, slot, seg], recv_sem.at[slot, seg])

    def part(way, slot, seg, side, g):
        return send(
            kv.at[slot, seg, side, g], way, far_send.at[way, seg, side, g], far_recv.at[seg, side, g]
        )

    def wanted(way, slot, seg, to):
        return (seg < 2) | ((slot < to) if way == 0 else (slot + 1 < half))

    def from_left(to, seg, side):
        if side == 0:
            return (to < half) | (to >= n - 2)
        return (to < half - 2) | ((to == n - 1) & (seg != 1))

    def last_hop(way, seg, side):
        return from_left(right, seg, side) if way == 0 else jnp.logical_not(from_left(left, seg, side))

    def send_own(seg):
        for way in range(2):
            @pl.when(wanted(way, me, seg, right))
            def _():
                ring(way, me, seg).start()

    for side in range(2):
        for g in range(groups):
            current(side, g).wait()
    pl.semaphore_wait(barrier, 2)
    send_own(2)

    for side in range(2):
        stored(side).wait()
        both = raw[side].astype(F32)
        for seg in range(2):
            for g in range(groups):
                kv[me, seg, side, g] = both[:, seg, g * HEAD : (g + 1) * HEAD].astype(BF16)

    for copy in small:
        copy.wait()

    def find(s, _):
        source_ref[s] = lax.fori_loop(
            0, n, lambda j, found: jnp.maximum(found, jnp.where(table_ref[j * n + me] == s, j, 0)), 0
        )
        return 0

    lax.fori_loop(0, n, find, 0)
    for seg in (1, 0):
        send_own(seg)

    lanes = lax.broadcasted_iota(jnp.int32, (QBLK, HEAD), 1)
    rising = lax.broadcasted_iota(jnp.int32, (QBLK, HEAD), 0)
    freq = freq_ref[...]
    all_queries.wait()

    def rotate(step, _):
        kind = step // (rows // QBLK)
        blk = lax.rem(step, rows // QBLK)
        angle = (rising + remap_ref[kind, blk]).astype(F32) * freq
        cos = jnp.cos(angle)
        sin = jnp.sin(angle)
        sin = jnp.where(lanes < HEAD // 2, -sin, sin)
        at = pl.ds(pl.multiple_of(blk * QBLK, QBLK), QBLK)
        for h in range(heads):
            x = q_ref[at, h * HEAD : (h + 1) * HEAD].astype(F32)
            turned = x * cos + pltpu.roll(x, HEAD // 2, 1) * sin
            qrot[2 - kind, h, at, :] = turned.astype(BF16)
        return 0

    lax.fori_loop(0, 3 * (rows // QBLK), rotate, 0)

    m_ref[...] = jnp.full_like(m_ref, MASKED)
    l_ref[...] = jnp.zeros_like(l_ref)
    acc[...] = jnp.zeros_like(acc)

    def attend(slots, seg, masked=False, finish=False, only=None):
        chosen = range(groups) if only is None else (only,)
        hs = range(chosen[0] * per, (chosen[-1] + 1) * per)
        keys = {g: [kv[slot, seg, 0, g] for slot in slots] for g in chosen}
        values = {g: [kv[slot, seg, 1, g].T for slot in slots] for g in chosen}
        if masked:
            key = lax.broadcasted_iota(jnp.int32, (rows, rows), 0)
            tok = lax.broadcasted_iota(jnp.int32, (rows, rows), 1)
            allowed = key <= tok

        def scores(h):
            q = qrot[seg, h]
            parts = [
                lax.dot_general(k, q, (((1,), (1,)), ((), ())), preferred_element_type=F32)
                for k in keys[h // per]
            ]
            return [jnp.where(allowed, s, MASKED) for s in parts] if masked else parts

        def gather(h, weights, alpha):
            parts = [
                jnp.dot(vt, p, preferred_element_type=F32)
                for vt, p in zip(values[h // per], weights)
            ]
            total = acc[h] * alpha + functools.reduce(jnp.add, parts)
            if finish:
                out_ref[:, h * HEAD : (h + 1) * HEAD] = (total / l_ref[h]).T.astype(BF16)
            else:
                acc[h] = total

        ahead, behind = scores(hs[0]), None
        for h in hs:
            now = ahead
            if h + 1 in hs:
                ahead = scores(h + 1)
            m_old = m_ref[h]
            m_new = jnp.maximum(
                m_old, jnp.max(functools.reduce(jnp.maximum, now), axis=0, keepdims=True)
            )
            alpha = jnp.exp2((m_old - m_new) * SCALE2)
            weights = [jnp.exp2((s - m_new) * SCALE2) for s in now]
            m_ref[h] = m_new
            l_ref[h] = l_ref[h] * alpha + jnp.sum(
                functools.reduce(jnp.add, weights), axis=0, keepdims=True
            )
            if behind is not None:
                gather(*behind)
            behind = (h, [p.astype(BF16) for p in weights], alpha)
        gather(*behind)

    page_rows = pl.ds(pl.multiple_of(me * PAGE, PAGE), PAGE)

    def keep_page(slot):
        for side in range(2):
            for g in range(groups):
                pages[slot, side, g] = kv[slot, 1, side, g, page_rows, :]

    def first(seg, _):
        attend((me,), seg)
        return 0

    keep_page(me)
    lax.fori_loop(0, 2, first, 0)
    attend((me,), 2, True)

    def step(t, _):
        up, down = lax.rem(me + n - t, n), lax.rem(me + t, n)

        def of_seg(i, _):
            seg = 2 - i
            for way in range(2):
                slot = (up, down)[way]

                @pl.when(wanted(way, slot, seg, me))
                def _():
                    ring(way, slot, seg).wait_recv()

                sends = wanted(way, slot, seg, right)

                @pl.when(sends & (t < half - 1))
                def _():
                    ring(way, slot, seg).start()

                for side in range(2):
                    @pl.when(sends & (t == half - 1) & last_hop(way, seg, side))
                    def _():
                        for g in range(groups):
                            part(way, slot, seg, side, g).start()

            @pl.when(seg == 1)
            def _():
                keep_page(up)
                keep_page(down)

            up_counts = (seg < 2) | (up < me)
            down_counts = (seg < 2) | (down < me)

            @pl.when(up_counts & down_counts)
            def _():
                attend((up, down), seg)

            @pl.when(up_counts != down_counts)
            def _():
                attend((jnp.where(up_counts, up, down),), seg)

            return 0

        lax.fori_loop(0, 3, of_seg, 0)
        return 0

    lax.fori_loop(1, half, step, 0)

    far = lax.rem(me + half, n)

    def last(i, _):
        seg = 2 - i

        @pl.when((seg < 2) | (far < me))
        def _():
            for side in range(2):
                for g in range(groups):
                    part(0, far, seg, side, g).wait_recv()
            attend((far,), seg)

        return 0

    lax.fori_loop(0, 2, last, 0)
    keep_page(far)

    def place(s, _):
        source = source_ref[s]
        at = pl.ds(pl.multiple_of(s * PAGE, PAGE), PAGE)
        for side in range(2):
            for g in range(groups):
                turned_pages[side, g, at, :] = pages[source, side, g].astype(F32)
        return 0

    lax.fori_loop(0, n, place, 0)
    for side, ref in enumerate((pk_ref, pv_ref)):
        for g in range(groups):
            for t in range(PAGE):
                ref[g, :, t * HEAD : (t + 1) * HEAD] = turned_pages[
                    side, g, pl.ds(t, n, stride=PAGE), :
                ].astype(BF16)

    for g in range(groups):
        for side in range(2):
            part(0, far, 0, side, g).wait_recv()
        attend((far,), 0, finish=True, only=g)

    def drain(t, _):
        def of_seg(seg, _):
            for way in range(2):
                slot = lax.rem(me + (n - t if way == 0 else t), n)
                sends = wanted(way, slot, seg, right)

                @pl.when(sends & (t < half - 1))
                def _():
                    ring(way, slot, seg).wait_send()

                for side in range(2):
                    @pl.when(sends & (t == half - 1) & last_hop(way, seg, side))
                    def _():
                        for g in range(groups):
                            part(way, slot, seg, side, g).wait_send()
            return 0

        lax.fori_loop(0, 3, of_seg, 0)
        return 0

    lax.fori_loop(0, half, drain, 0)


def finish_kernel(a_ref, k_ref, v_ref, a_out, k_out, v_out, sem):
    copies = [
        pltpu.make_async_copy(src, dst, sem.at[i])
        for i, (src, dst) in enumerate(((a_ref, a_out), (k_ref, k_out), (v_ref, v_out)))
    ]
    for copy in copies:
        copy.start()
    for copy in copies:
        copy.wait()


def shards(queries, current_keys, current_values, stored_keys, stored_values, remap_table, block_table, *, n):
    rows = queries.shape[0]
    groups = current_keys.shape[1] // HEAD
    heads = queries.shape[1] // HEAD
    d = np.arange(HEAD // 2, dtype=np.float32)
    freq = (np.float32(ROPE_BASE) ** (np.float32(-2.0) * d / np.float32(HEAD))).astype(np.float32)
    freq = jnp.asarray(np.concatenate([freq, freq])[None, :])
    vmem = pl.BlockSpec(memory_space=pltpu.VMEM)
    hbm = pl.BlockSpec(memory_space=pltpu.HBM)
    paged = pltpu.VMEM((groups, n, PAGE * HEAD), BF16)
    results = pl.pallas_call(
        functools.partial(kernel, n, groups, heads // groups),
        out_shape=(pltpu.VMEM(queries.shape, BF16), paged, paged),
        in_specs=[hbm] * 8,
        out_specs=(vmem, vmem, vmem),
        scratch_shapes=[
            pltpu.SMEM(block_table.shape, jnp.int32),
            pltpu.SMEM(remap_table.shape, jnp.int32),
            pltpu.VMEM(freq.shape, F32),
            pltpu.VMEM((n, 3, 2, groups, rows, HEAD), BF16),
            pltpu.VMEM(queries.shape, BF16),
            pltpu.VMEM((2, *stored_keys.shape), BF16),
            pltpu.VMEM((3, heads, rows, HEAD), BF16),
            pltpu.VMEM((heads, HEAD, rows), F32),
            pltpu.VMEM((heads, 1, rows), F32),
            pltpu.VMEM((heads, 1, rows), F32),
            pltpu.VMEM((n, 2, groups, PAGE, HEAD), BF16),
            pltpu.VMEM((2, groups, n * PAGE, HEAD), F32),
            pltpu.SMEM((n,), jnp.int32),
            pltpu.SemaphoreType.DMA((3,)),
            pltpu.SemaphoreType.DMA((2, groups)),
            pltpu.SemaphoreType.DMA((2,)),
            pltpu.SemaphoreType.DMA,
            pltpu.SemaphoreType.DMA((2, n, 3)),
            pltpu.SemaphoreType.DMA((n, 3)),
            pltpu.SemaphoreType.DMA((2, 3, 2, groups)),
            pltpu.SemaphoreType.DMA((3, 2, groups)),
        ],
        compiler_params=pltpu.CompilerParams(
            collective_id=0, has_side_effects=True, vmem_limit_bytes=58 * 1024 * 1024
        ),
    )(
        block_table, remap_table, freq, queries,
        stored_keys, stored_values, current_keys, current_values,
    )
    return pl.pallas_call(
        finish_kernel,
        out_shape=tuple(jax.ShapeDtypeStruct(r.shape, BF16) for r in results),
        in_specs=[vmem] * 3,
        out_specs=(hbm, hbm, hbm),
        scratch_shapes=[pltpu.SemaphoreType.DMA((3,))],
        compiler_params=pltpu.CompilerParams(vmem_limit_bytes=4 * 1024 * 1024),
    )(*results)


def solution(mesh):
    both = ("groups", "seq")
    in_specs = (
        P(both, "head"), P(both, "head"), P(both, "head"),
        P(both, None, "head"), P(both, None, "head"),
        P(None, both), P("groups"),
    )
    out_specs = (P(both, "head"), P("head", both, None), P("head", both, None))
    return jax.shard_map(
        functools.partial(shards, n=mesh.shape["seq"]),
        mesh=mesh, in_specs=in_specs, out_specs=out_specs, check_vma=False,
    )
```

```python
import functools

import jax
import jax.numpy as jnp
import numpy as np
from jax import lax
from jax.experimental import pallas as pl
from jax.experimental.pallas import tpu as pltpu
from jax.sharding import PartitionSpec as P

HEAD = 128
PAGE = 16
QBLK = 64
ROPE_BASE = 1000000.0
MASKED = -1e30
MESH = pl.DeviceIdType.MESH
F32 = jnp.float32
BF16 = jnp.bfloat16
SCALE2 = float(HEAD**-0.5 * np.log2(np.e))


def kernel(
    n, groups, per,
    table_hbm, remap_hbm, freq_hbm, q_hbm, sk_hbm, sv_hbm, ck_hbm, cv_hbm,
    out_ref, pk_ref, pv_ref,
    table_ref, remap_ref, freq_ref, kv, q_ref, raw, qrot, acc, m_ref, l_ref, pages, turned_pages, source_ref,
    small_sem, own_sem, raw_sem, q_sem, send_sem, recv_sem, far_send, far_recv,
):
    me = lax.axis_index("seq")
    half = n // 2
    rows = q_ref.shape[0]
    heads = groups * per
    right, left = lax.rem(me + 1, n), lax.rem(me + n - 1, n)

    def current(side, g):
        return pltpu.make_async_copy(
            (ck_hbm, cv_hbm)[side].at[:, pl.ds(g * HEAD, HEAD)], kv.at[me, 2, side, g], own_sem.at[side, g]
        )

    def stored(side):
        return pltpu.make_async_copy((sk_hbm, sv_hbm)[side], raw.at[side], raw_sem.at[side])

    all_queries = pltpu.make_async_copy(q_hbm, q_ref, q_sem)
    small = [
        pltpu.make_async_copy(src, dst, small_sem.at[i])
        for i, (src, dst) in enumerate(
            ((table_hbm, table_ref), (remap_hbm, remap_ref), (freq_hbm, freq_ref))
        )
    ]

    barrier = pltpu.get_barrier_semaphore()
    for neighbour in (left, right):
        pl.semaphore_signal(barrier, inc=1, device_id={"seq": neighbour}, device_id_type=MESH)
    for side in range(2):
        for g in range(groups):
            current(side, g).start()
    for side in range(2):
        stored(side).start()
    for copy in small:
        copy.start()
    all_queries.start()

    def send(unit, way, send_sem, recv_sem):
        return pltpu.make_async_remote_copy(
            src_ref=unit,
            dst_ref=unit,
            send_sem=send_sem,
            recv_sem=recv_sem,
            device_id={"seq": (right, left)[way]},
            device_id_type=MESH,
        )

    def ring(way, slot, seg):
        return send(kv.at[slot, seg], way, send_sem.at[way, slot, seg], recv_sem.at[slot, seg])

    def part(way, slot, seg, side, g):
        return send(
            kv.at[slot, seg, side, g], way, far_send.at[way, seg, side, g], far_recv.at[seg, side, g]
        )

    def wanted(way, slot, seg, to):
        return (seg < 2) | ((slot < to) if way == 0 else (slot + 1 < half))

    def from_left(to, seg, side):
        if side == 0:
            return to >= n - 2
        return (to == n - 1) & (seg != 1)

    def last_hop(way, seg, side):
        return from_left(right, seg, side) if way == 0 else jnp.logical_not(from_left(left, seg, side))

    def send_own(seg):
        for way in range(2):
            @pl.when(wanted(way, me, seg, right))
            def _():
                ring(way, me, seg).start()

    for side in range(2):
        for g in range(groups):
            current(side, g).wait()
    pl.semaphore_wait(barrier, 2)
    send_own(2)

    for side in range(2):
        stored(side).wait()
        both = raw[side].astype(F32)
        for seg in range(2):
            for g in range(groups):
                kv[me, seg, side, g] = both[:, seg, g * HEAD : (g + 1) * HEAD].astype(BF16)

    for copy in small:
        copy.wait()

    def find(s, _):
        source_ref[s] = lax.fori_loop(
            0, n, lambda j, found: jnp.maximum(found, jnp.where(table_ref[j * n + me] == s, j, 0)), 0
        )
        return 0

    lax.fori_loop(0, n, find, 0)
    for seg in (1, 0):
        send_own(seg)

    lanes = lax.broadcasted_iota(jnp.int32, (QBLK, HEAD), 1)
    rising = lax.broadcasted_iota(jnp.int32, (QBLK, HEAD), 0)
    freq = freq_ref[...]
    all_queries.wait()

    def rotate(step, _):
        kind = step // (rows // QBLK)
        blk = lax.rem(step, rows // QBLK)
        angle = (rising + remap_ref[kind, blk]).astype(F32) * freq
        cos = jnp.cos(angle)
        sin = jnp.sin(angle)
        sin = jnp.where(lanes < HEAD // 2, -sin, sin)
        at = pl.ds(pl.multiple_of(blk * QBLK, QBLK), QBLK)
        for h in range(heads):
            x = q_ref[at, h * HEAD : (h + 1) * HEAD].astype(F32)
            turned = x * cos + pltpu.roll(x, HEAD // 2, 1) * sin
            qrot[2 - kind, h, at, :] = turned.astype(BF16)
        return 0

    lax.fori_loop(0, 3 * (rows // QBLK), rotate, 0)

    m_ref[...] = jnp.full_like(m_ref, MASKED)
    l_ref[...] = jnp.zeros_like(l_ref)
    acc[...] = jnp.zeros_like(acc)

    def attend(slots, seg, masked=False, finish=False, only=None):
        chosen = range(groups) if only is None else (only,)
        hs = range(chosen[0] * per, (chosen[-1] + 1) * per)
        keys = {g: [kv[slot, seg, 0, g] for slot in slots] for g in chosen}
        values = {g: [kv[slot, seg, 1, g].T for slot in slots] for g in chosen}
        if masked:
            key = lax.broadcasted_iota(jnp.int32, (rows, rows), 0)
            tok = lax.broadcasted_iota(jnp.int32, (rows, rows), 1)
            allowed = key <= tok

        def scores(h):
            q = qrot[seg, h]
            parts = [
                lax.dot_general(k, q, (((1,), (1,)), ((), ())), preferred_element_type=F32)
                for k in keys[h // per]
            ]
            return [jnp.where(allowed, s, MASKED) for s in parts] if masked else parts

        def gather(h, weights, alpha):
            parts = [
                jnp.dot(vt, p, preferred_element_type=F32)
                for vt, p in zip(values[h // per], weights)
            ]
            total = acc[h] * alpha + functools.reduce(jnp.add, parts)
            if finish:
                out_ref[:, h * HEAD : (h + 1) * HEAD] = (total / l_ref[h]).T.astype(BF16)
            else:
                acc[h] = total

        ahead, behind = scores(hs[0]), None
        for h in hs:
            now = ahead
            if h + 1 in hs:
                ahead = scores(h + 1)
            m_old = m_ref[h]
            m_new = jnp.maximum(
                m_old, jnp.max(functools.reduce(jnp.maximum, now), axis=0, keepdims=True)
            )
            alpha = jnp.exp2((m_old - m_new) * SCALE2)
            weights = [jnp.exp2((s - m_new) * SCALE2) for s in now]
            m_ref[h] = m_new
            l_ref[h] = l_ref[h] * alpha + jnp.sum(
                functools.reduce(jnp.add, weights), axis=0, keepdims=True
            )
            if behind is not None:
                gather(*behind)
            behind = (h, [p.astype(BF16) for p in weights], alpha)
        gather(*behind)

    page_rows = pl.ds(pl.multiple_of(me * PAGE, PAGE), PAGE)

    def keep_page(slot):
        for side in range(2):
            for g in range(groups):
                pages[slot, side, g] = kv[slot, 1, side, g, page_rows, :]

    def first(seg, _):
        attend((me,), seg)
        return 0

    keep_page(me)
    lax.fori_loop(0, 2, first, 0)
    attend((me,), 2, True)

    def step(t, _):
        up, down = lax.rem(me + n - t, n), lax.rem(me + t, n)

        def of_seg(i, _):
            seg = 2 - i
            for way in range(2):
                slot = (up, down)[way]

                @pl.when(wanted(way, slot, seg, me))
                def _():
                    ring(way, slot, seg).wait_recv()

                sends = wanted(way, slot, seg, right)

                @pl.when(sends & (t < half - 1))
                def _():
                    ring(way, slot, seg).start()

                for side in range(2):
                    @pl.when(sends & (t == half - 1) & last_hop(way, seg, side))
                    def _():
                        for g in range(groups):
                            part(way, slot, seg, side, g).start()

            @pl.when(seg == 1)
            def _():
                keep_page(up)
                keep_page(down)

            up_counts = (seg < 2) | (up < me)
            down_counts = (seg < 2) | (down < me)

            @pl.when(up_counts & down_counts)
            def _():
                attend((up, down), seg)

            @pl.when(up_counts != down_counts)
            def _():
                attend((jnp.where(up_counts, up, down),), seg)

            return 0

        lax.fori_loop(0, 3, of_seg, 0)
        return 0

    lax.fori_loop(1, half, step, 0)

    far = lax.rem(me + half, n)

    def last(i, _):
        seg = 2 - i

        @pl.when((seg < 2) | (far < me))
        def _():
            for side in range(2):
                for g in range(groups):
                    part(0, far, seg, side, g).wait_recv()
            attend((far,), seg)

        return 0

    lax.fori_loop(0, 2, last, 0)
    keep_page(far)

    def place(s, _):
        source = source_ref[s]
        at = pl.ds(pl.multiple_of(s * PAGE, PAGE), PAGE)
        for side in range(2):
            for g in range(groups):
                turned_pages[side, g, at, :] = pages[source, side, g].astype(F32)
        return 0

    lax.fori_loop(0, n, place, 0)
    for side, ref in enumerate((pk_ref, pv_ref)):
        for g in range(groups):
            for t in range(PAGE):
                ref[g, :, t * HEAD : (t + 1) * HEAD] = turned_pages[
                    side, g, pl.ds(t, n, stride=PAGE), :
                ].astype(BF16)

    for g in range(groups):
        for side in range(2):
            part(0, far, 0, side, g).wait_recv()
        attend((far,), 0, finish=True, only=g)

    def drain(t, _):
        def of_seg(seg, _):
            for way in range(2):
                slot = lax.rem(me + (n - t if way == 0 else t), n)
                sends = wanted(way, slot, seg, right)

                @pl.when(sends & (t < half - 1))
                def _():
                    ring(way, slot, seg).wait_send()

                for side in range(2):
                    @pl.when(sends & (t == half - 1) & last_hop(way, seg, side))
                    def _():
                        for g in range(groups):
                            part(way, slot, seg, side, g).wait_send()
            return 0

        lax.fori_loop(0, 3, of_seg, 0)
        return 0

    lax.fori_loop(0, half, drain, 0)


def finish_kernel(a_ref, k_ref, v_ref, a_out, k_out, v_out, sem):
    copies = [
        pltpu.make_async_copy(src, dst, sem.at[i])
        for i, (src, dst) in enumerate(((a_ref, a_out), (k_ref, k_out), (v_ref, v_out)))
    ]
    for copy in copies:
        copy.start()
    for copy in copies:
        copy.wait()


def shards(queries, current_keys, current_values, stored_keys, stored_values, remap_table, block_table, *, n):
    rows = queries.shape[0]
    groups = current_keys.shape[1] // HEAD
    heads = queries.shape[1] // HEAD
    d = np.arange(HEAD // 2, dtype=np.float32)
    freq = (np.float32(ROPE_BASE) ** (np.float32(-2.0) * d / np.float32(HEAD))).astype(np.float32)
    freq = jnp.asarray(np.concatenate([freq, freq])[None, :])
    vmem = pl.BlockSpec(memory_space=pltpu.VMEM)
    hbm = pl.BlockSpec(memory_space=pltpu.HBM)
    paged = pltpu.VMEM((groups, n, PAGE * HEAD), BF16)
    results = pl.pallas_call(
        functools.partial(kernel, n, groups, heads // groups),
        out_shape=(pltpu.VMEM(queries.shape, BF16), paged, paged),
        in_specs=[hbm] * 8,
        out_specs=(vmem, vmem, vmem),
        scratch_shapes=[
            pltpu.SMEM(block_table.shape, jnp.int32),
            pltpu.SMEM(remap_table.shape, jnp.int32),
            pltpu.VMEM(freq.shape, F32),
            pltpu.VMEM((n, 3, 2, groups, rows, HEAD), BF16),
            pltpu.VMEM(queries.shape, BF16),
            pltpu.VMEM((2, *stored_keys.shape), BF16),
            pltpu.VMEM((3, heads, rows, HEAD), BF16),
            pltpu.VMEM((heads, HEAD, rows), F32),
            pltpu.VMEM((heads, 1, rows), F32),
            pltpu.VMEM((heads, 1, rows), F32),
            pltpu.VMEM((n, 2, groups, PAGE, HEAD), BF16),
            pltpu.VMEM((2, groups, n * PAGE, HEAD), F32),
            pltpu.SMEM((n,), jnp.int32),
            pltpu.SemaphoreType.DMA((3,)),
            pltpu.SemaphoreType.DMA((2, groups)),
            pltpu.SemaphoreType.DMA((2,)),
            pltpu.SemaphoreType.DMA,
            pltpu.SemaphoreType.DMA((2, n, 3)),
            pltpu.SemaphoreType.DMA((n, 3)),
            pltpu.SemaphoreType.DMA((2, 3, 2, groups)),
            pltpu.SemaphoreType.DMA((3, 2, groups)),
        ],
        compiler_params=pltpu.CompilerParams(
            collective_id=0, has_side_effects=True, vmem_limit_bytes=58 * 1024 * 1024
        ),
    )(
        block_table, remap_table, freq, queries,
        stored_keys, stored_values, current_keys, current_values,
    )
    return pl.pallas_call(
        finish_kernel,
        out_shape=tuple(jax.ShapeDtypeStruct(r.shape, BF16) for r in results),
        in_specs=[vmem] * 3,
        out_specs=(hbm, hbm, hbm),
        scratch_shapes=[pltpu.SemaphoreType.DMA((3,))],
        compiler_params=pltpu.CompilerParams(vmem_limit_bytes=4 * 1024 * 1024),
    )(*results)


def solution(mesh):
    both = ("groups", "seq")
    in_specs = (
        P(both, "head"), P(both, "head"), P(both, "head"),
        P(both, None, "head"), P(both, None, "head"),
        P(None, both), P("groups"),
    )
    out_specs = (P(both, "head"), P("head", both, None), P("head", both, None))
    return jax.shard_map(
        functools.partial(shards, n=mesh.shape["seq"]),
        mesh=mesh, in_specs=in_specs, out_specs=out_specs, check_vma=False,
    )
```

```python
import functools

import jax
import jax.numpy as jnp
import numpy as np
from jax import lax
from jax.experimental import pallas as pl
from jax.experimental.pallas import tpu as pltpu
from jax.sharding import PartitionSpec as P

HEAD = 128
PAGE = 16
QBLK = 64
ROPE_BASE = 1000000.0
MASKED = -1e30
MESH = pl.DeviceIdType.MESH
F32 = jnp.float32
BF16 = jnp.bfloat16
SCALE2 = float(HEAD**-0.5 * np.log2(np.e))


def kernel(
    n, groups, per,
    table_hbm, remap_hbm, freq_hbm, q_hbm, sk_hbm, sv_hbm, ck_hbm, cv_hbm,
    out_ref, pk_ref, pv_ref,
    table_ref, remap_ref, freq_ref, kv, q_ref, raw, qrot, acc, m_ref, l_ref, pages, turned_pages, source_ref,
    small_sem, own_sem, raw_sem, q_sem, send_sem, recv_sem, far_send, far_recv,
):
    me = lax.axis_index("seq")
    half = n // 2
    rows = q_ref.shape[0]
    heads = groups * per
    right, left = lax.rem(me + 1, n), lax.rem(me + n - 1, n)

    def current(side, g):
        return pltpu.make_async_copy(
            (ck_hbm, cv_hbm)[side].at[:, pl.ds(g * HEAD, HEAD)], kv.at[me, 2, side, g], own_sem.at[side, g]
        )

    def stored(side):
        return pltpu.make_async_copy((sk_hbm, sv_hbm)[side], raw.at[side], raw_sem.at[side])

    all_queries = pltpu.make_async_copy(q_hbm, q_ref, q_sem)
    small = [
        pltpu.make_async_copy(src, dst, small_sem.at[i])
        for i, (src, dst) in enumerate(
            ((table_hbm, table_ref), (remap_hbm, remap_ref), (freq_hbm, freq_ref))
        )
    ]

    barrier = pltpu.get_barrier_semaphore()
    for neighbour in (left, right):
        pl.semaphore_signal(barrier, inc=1, device_id={"seq": neighbour}, device_id_type=MESH)
    for side in range(2):
        for g in range(groups):
            current(side, g).start()
    for side in range(2):
        stored(side).start()
    for copy in small:
        copy.start()
    all_queries.start()

    def send(unit, way, send_sem, recv_sem):
        return pltpu.make_async_remote_copy(
            src_ref=unit,
            dst_ref=unit,
            send_sem=send_sem,
            recv_sem=recv_sem,
            device_id={"seq": (right, left)[way]},
            device_id_type=MESH,
        )

    def ring(way, slot, seg):
        return send(kv.at[slot, seg], way, send_sem.at[way, slot, seg], recv_sem.at[slot, seg])

    def part(way, slot, seg, side, g):
        return send(
            kv.at[slot, seg, side, g], way, far_send.at[way, seg, side, g], far_recv.at[seg, side, g]
        )

    def wanted(way, slot, seg, to):
        return (seg < 2) | ((slot < to) if way == 0 else (slot + 1 < half))

    def from_left(to, seg, side, g):
        if side == 0:
            return to >= n - 2
        return (to == n - 1) & ((seg == 2) | (seg == 0) if g == 0 else (seg == 2))

    def last_hop(way, seg, side, g):
        if way == 0:
            return from_left(right, seg, side, g)
        return jnp.logical_not(from_left(left, seg, side, g))

    def send_own(seg):
        for way in range(2):
            @pl.when(wanted(way, me, seg, right))
            def _():
                ring(way, me, seg).start()

    for side in range(2):
        for g in range(groups):
            current(side, g).wait()
    pl.semaphore_wait(barrier, 2)
    send_own(2)

    for side in range(2):
        stored(side).wait()
        both = raw[side].astype(F32)
        for seg in range(2):
            for g in range(groups):
                kv[me, seg, side, g] = both[:, seg, g * HEAD : (g + 1) * HEAD].astype(BF16)

    for copy in small:
        copy.wait()

    def find(s, _):
        source_ref[s] = lax.fori_loop(
            0, n, lambda j, found: jnp.maximum(found, jnp.where(table_ref[j * n + me] == s, j, 0)), 0
        )
        return 0

    lax.fori_loop(0, n, find, 0)
    for seg in (1, 0):
        send_own(seg)

    lanes = lax.broadcasted_iota(jnp.int32, (QBLK, HEAD), 1)
    rising = lax.broadcasted_iota(jnp.int32, (QBLK, HEAD), 0)
    freq = freq_ref[...]
    all_queries.wait()

    def rotate(step, _):
        kind = step // (rows // QBLK)
        blk = lax.rem(step, rows // QBLK)
        angle = (rising + remap_ref[kind, blk]).astype(F32) * freq
        cos = jnp.cos(angle)
        sin = jnp.sin(angle)
        sin = jnp.where(lanes < HEAD // 2, -sin, sin)
        at = pl.ds(pl.multiple_of(blk * QBLK, QBLK), QBLK)
        for h in range(heads):
            x = q_ref[at, h * HEAD : (h + 1) * HEAD].astype(F32)
            turned = x * cos + pltpu.roll(x, HEAD // 2, 1) * sin
            qrot[2 - kind, h, at, :] = turned.astype(BF16)
        return 0

    lax.fori_loop(0, 3 * (rows // QBLK), rotate, 0)

    m_ref[...] = jnp.full_like(m_ref, MASKED)
    l_ref[...] = jnp.zeros_like(l_ref)
    acc[...] = jnp.zeros_like(acc)

    def attend(slots, seg, masked=False, finish=False, only=None):
        chosen = range(groups) if only is None else (only,)
        hs = range(chosen[0] * per, (chosen[-1] + 1) * per)
        keys = {g: [kv[slot, seg, 0, g] for slot in slots] for g in chosen}
        values = {g: [kv[slot, seg, 1, g].T for slot in slots] for g in chosen}
        if masked:
            key = lax.broadcasted_iota(jnp.int32, (rows, rows), 0)
            tok = lax.broadcasted_iota(jnp.int32, (rows, rows), 1)
            allowed = key <= tok

        def scores(h):
            q = qrot[seg, h]
            parts = [
                lax.dot_general(k, q, (((1,), (1,)), ((), ())), preferred_element_type=F32)
                for k in keys[h // per]
            ]
            return [jnp.where(allowed, s, MASKED) for s in parts] if masked else parts

        def gather(h, weights, alpha):
            parts = [
                jnp.dot(vt, p, preferred_element_type=F32)
                for vt, p in zip(values[h // per], weights)
            ]
            total = acc[h] * alpha + functools.reduce(jnp.add, parts)
            if finish:
                out_ref[:, h * HEAD : (h + 1) * HEAD] = (total / l_ref[h]).T.astype(BF16)
            else:
                acc[h] = total

        ahead, behind = scores(hs[0]), None
        for h in hs:
            now = ahead
            if h + 1 in hs:
                ahead = scores(h + 1)
            m_old = m_ref[h]
            m_new = jnp.maximum(
                m_old, jnp.max(functools.reduce(jnp.maximum, now), axis=0, keepdims=True)
            )
            alpha = jnp.exp2((m_old - m_new) * SCALE2)
            weights = [jnp.exp2((s - m_new) * SCALE2) for s in now]
            m_ref[h] = m_new
            l_ref[h] = l_ref[h] * alpha + jnp.sum(
                functools.reduce(jnp.add, weights), axis=0, keepdims=True
            )
            if behind is not None:
                gather(*behind)
            behind = (h, [p.astype(BF16) for p in weights], alpha)
        gather(*behind)

    page_rows = pl.ds(pl.multiple_of(me * PAGE, PAGE), PAGE)

    def keep_page(slot):
        for side in range(2):
            for g in range(groups):
                pages[slot, side, g] = kv[slot, 1, side, g, page_rows, :]

    def first(seg, _):
        attend((me,), seg)
        return 0

    keep_page(me)
    lax.fori_loop(0, 2, first, 0)
    attend((me,), 2, True)

    def step(t, _):
        up, down = lax.rem(me + n - t, n), lax.rem(me + t, n)

        def of_seg(i, _):
            seg = 2 - i
            for way in range(2):
                slot = (up, down)[way]

                @pl.when(wanted(way, slot, seg, me))
                def _():
                    ring(way, slot, seg).wait_recv()

                sends = wanted(way, slot, seg, right)

                @pl.when(sends & (t < half - 1))
                def _():
                    ring(way, slot, seg).start()

                for side in range(2):
                    for g in reversed(range(groups)):
                        @pl.when(sends & (t == half - 1) & last_hop(way, seg, side, g))
                        def _():
                            part(way, slot, seg, side, g).start()

            @pl.when(seg == 1)
            def _():
                keep_page(up)
                keep_page(down)

            up_counts = (seg < 2) | (up < me)
            down_counts = (seg < 2) | (down < me)

            @pl.when(up_counts & down_counts)
            def _():
                attend((up, down), seg)

            @pl.when(up_counts != down_counts)
            def _():
                attend((jnp.where(up_counts, up, down),), seg)

            return 0

        lax.fori_loop(0, 3, of_seg, 0)
        return 0

    lax.fori_loop(1, half, step, 0)

    far = lax.rem(me + half, n)

    def last(i, _):
        seg = 2 - i

        @pl.when((seg < 2) | (far < me))
        def _():
            for side in range(2):
                for g in range(groups):
                    part(0, far, seg, side, g).wait_recv()
            attend((far,), seg)

        return 0

    lax.fori_loop(0, 2, last, 0)
    keep_page(far)

    def place(s, _):
        source = source_ref[s]
        at = pl.ds(pl.multiple_of(s * PAGE, PAGE), PAGE)
        for side in range(2):
            for g in range(groups):
                turned_pages[side, g, at, :] = pages[source, side, g].astype(F32)
        return 0

    lax.fori_loop(0, n, place, 0)
    for side, ref in enumerate((pk_ref, pv_ref)):
        for g in range(groups):
            for t in range(PAGE):
                ref[g, :, t * HEAD : (t + 1) * HEAD] = turned_pages[
                    side, g, pl.ds(t, n, stride=PAGE), :
                ].astype(BF16)

    for g in reversed(range(groups)):
        for side in range(2):
            part(0, far, 0, side, g).wait_recv()
        attend((far,), 0, finish=True, only=g)

    def drain(t, _):
        def of_seg(seg, _):
            for way in range(2):
                slot = lax.rem(me + (n - t if way == 0 else t), n)
                sends = wanted(way, slot, seg, right)

                @pl.when(sends & (t < half - 1))
                def _():
                    ring(way, slot, seg).wait_send()

                for side in range(2):
                    for g in range(groups):
                        @pl.when(sends & (t == half - 1) & last_hop(way, seg, side, g))
                        def _():
                            part(way, slot, seg, side, g).wait_send()
            return 0

        lax.fori_loop(0, 3, of_seg, 0)
        return 0

    lax.fori_loop(0, half, drain, 0)


def finish_kernel(a_ref, k_ref, v_ref, a_out, k_out, v_out, sem):
    copies = [
        pltpu.make_async_copy(src, dst, sem.at[i])
        for i, (src, dst) in enumerate(((a_ref, a_out), (k_ref, k_out), (v_ref, v_out)))
    ]
    for copy in copies:
        copy.start()
    for copy in copies:
        copy.wait()


def shards(queries, current_keys, current_values, stored_keys, stored_values, remap_table, block_table, *, n):
    rows = queries.shape[0]
    groups = current_keys.shape[1] // HEAD
    heads = queries.shape[1] // HEAD
    d = np.arange(HEAD // 2, dtype=np.float32)
    freq = (np.float32(ROPE_BASE) ** (np.float32(-2.0) * d / np.float32(HEAD))).astype(np.float32)
    freq = jnp.asarray(np.concatenate([freq, freq])[None, :])
    vmem = pl.BlockSpec(memory_space=pltpu.VMEM)
    hbm = pl.BlockSpec(memory_space=pltpu.HBM)
    paged = pltpu.VMEM((groups, n, PAGE * HEAD), BF16)
    results = pl.pallas_call(
        functools.partial(kernel, n, groups, heads // groups),
        out_shape=(pltpu.VMEM(queries.shape, BF16), paged, paged),
        in_specs=[hbm] * 8,
        out_specs=(vmem, vmem, vmem),
        scratch_shapes=[
            pltpu.SMEM(block_table.shape, jnp.int32),
            pltpu.SMEM(remap_table.shape, jnp.int32),
            pltpu.VMEM(freq.shape, F32),
            pltpu.VMEM((n, 3, 2, groups, rows, HEAD), BF16),
            pltpu.VMEM(queries.shape, BF16),
            pltpu.VMEM((2, *stored_keys.shape), BF16),
            pltpu.VMEM((3, heads, rows, HEAD), BF16),
            pltpu.VMEM((heads, HEAD, rows), F32),
            pltpu.VMEM((heads, 1, rows), F32),
            pltpu.VMEM((heads, 1, rows), F32),
            pltpu.VMEM((n, 2, groups, PAGE, HEAD), BF16),
            pltpu.VMEM((2, groups, n * PAGE, HEAD), F32),
            pltpu.SMEM((n,), jnp.int32),
            pltpu.SemaphoreType.DMA((3,)),
            pltpu.SemaphoreType.DMA((2, groups)),
            pltpu.SemaphoreType.DMA((2,)),
            pltpu.SemaphoreType.DMA,
            pltpu.SemaphoreType.DMA((2, n, 3)),
            pltpu.SemaphoreType.DMA((n, 3)),
            pltpu.SemaphoreType.DMA((2, 3, 2, groups)),
            pltpu.SemaphoreType.DMA((3, 2, groups)),
        ],
        compiler_params=pltpu.CompilerParams(
            collective_id=0, has_side_effects=True, vmem_limit_bytes=58 * 1024 * 1024
        ),
    )(
        block_table, remap_table, freq, queries,
        stored_keys, stored_values, current_keys, current_values,
    )
    return pl.pallas_call(
        finish_kernel,
        out_shape=tuple(jax.ShapeDtypeStruct(r.shape, BF16) for r in results),
        in_specs=[vmem] * 3,
        out_specs=(hbm, hbm, hbm),
        scratch_shapes=[pltpu.SemaphoreType.DMA((3,))],
        compiler_params=pltpu.CompilerParams(vmem_limit_bytes=4 * 1024 * 1024),
    )(*results)


def solution(mesh):
    both = ("groups", "seq")
    in_specs = (
        P(both, "head"), P(both, "head"), P(both, "head"),
        P(both, None, "head"), P(both, None, "head"),
        P(None, both), P("groups"),
    )
    out_specs = (P(both, "head"), P("head", both, None), P("head", both, None))
    return jax.shard_map(
        functools.partial(shards, n=mesh.shape["seq"]),
        mesh=mesh, in_specs=in_specs, out_specs=out_specs, check_vma=False,
    )
```
